32 devices in a mesh: groups: 2 (over x), head: 8 (over z, y), batch: 2 (over core).
Axes of the slice: x: 2, y: 2, z: 4, core: 2. Of those that a mesh axis runs over, the one named last changes fastest.
Arguments:
- latent_rows: bfloat16 [4096, 576], P(('groups', 'batch', 'head')), parts along dimension 0, may hold values from -6 to 6
- pre_queries: bfloat16 [4096, 128, 192], P(('groups', 'batch'), 'head'), parts along dimension 0, may hold values from -270 to 270
- pre_lengths: int32 [4, 4], P('groups'), parts along dimension 0, may hold values from 1 to 512, 1024 in all within a row
- owner_map: int32 [4, 4], P('groups'), parts along dimension 0, may hold values from 0 to 31, as said below
- context_cache: bfloat16 [64, 4096, 576], P(('groups', 'batch', 'head')), parts along dimension 0, may hold values from -6 to 6
- context_lengths: int32 [64], P(('groups', 'batch', 'head')), parts along dimension 0, may hold values from 1 to 4096, 65536 in all
- new_latent: bfloat16 [4, 32, 576], P('groups', ('batch', 'head')), parts along dimension 0, may hold values from -6 to 6
- dec_queries: bfloat16 [4, 32, 128, 192], P('groups', 'batch', 'head'), parts along dimension 0, may hold values from -270 to 270
- key_weight: bfloat16 [512, 16384], P(None, 'head'), may hold values from -0.25 to 0.25
- value_weight: bfloat16 [512, 16384], P(None, 'head'), may hold values from -0.25 to 0.25
Outputs:
- prefill_out: bfloat16 [4096, 16384], P(('groups', 'batch'), 'head'), parts along dimension 0
- decode_out: bfloat16 [4, 32, 16384], P('groups', 'batch', 'head'), parts along dimension 0
The draws below stay inside these ranges and needn't reach their ends.
There are 2 independent parts, one for each index of `groups`. The reference program is written for one: setup_inputs(seed, part) draws one part's arguments, and reference() takes and returns one part's arrays. A program takes and returns all parts, laid end to end along the dimension named above; an argument that names none is the same for every part. Nothing has to cross between parts.
Inputs may be any that keep to these rules, and one draw needn't show every extreme that they name: `owner_map`: the entries are distinct decode requests.
All inputs are finite; a program needn't handle non-finite values. No bound on the sum of `context_lengths` on one device may be relied on, other than what follows from the above.
Results may differ from the reference program's by a relative error of at most 0.0061.
Values may be sent and summed in bfloat16 or wider, within the bound.
A program may use at most 192 MiB of HBM per device.

```python
import math
import jax
import jax.numpy as jnp
import numpy as np
from jax import lax

H = 128
HD = 128
ROPE = 64
LAT = 512
KV = 576
PRE = 1024
SEGS = 4
PMOST = 512
CTX = 4096
STEPS = 2
SPANS = 2
REQS = 32


def clipped_normal(key, salt, shape):
    return jnp.clip(jax.random.normal(jax.random.fold_in(key, salt), shape, jnp.float32), -6.0, 6.0)


def draw_latent_rows(key, part):
    latent = clipped_normal(key, 11, (SPANS * PRE, LAT))
    rope_part = clipped_normal(key, 12, (SPANS * PRE, ROPE))
    return jnp.concatenate([latent, rope_part], axis=1).astype(jnp.bfloat16)


def draw_pre_queries(key, part):
    drawn_part = clipped_normal(key, 13, (SPANS * PRE, H, HD))
    rope_part = clipped_normal(key, 14, (SPANS * PRE, H, ROPE))
    return jnp.concatenate([drawn_part, rope_part], axis=2).astype(jnp.bfloat16)


def draw_new_latent(key, part):
    latent = clipped_normal(key, 21, (STEPS, REQS, LAT))
    rope_part = clipped_normal(key, 22, (STEPS, REQS, ROPE))
    return jnp.concatenate([latent, rope_part], axis=2).astype(jnp.bfloat16)


def draw_dec_queries(key, part):
    drawn_part = clipped_normal(key, 23, (STEPS, REQS, H, HD))
    rope_part = clipped_normal(key, 24, (STEPS, REQS, H, ROPE))
    return jnp.concatenate([drawn_part, rope_part], axis=3).astype(jnp.bfloat16)


def draw_owner_map(key, part):
    middle = jax.random.permutation(jax.random.fold_in(key, 31), REQS - 2) + 1
    picked = jnp.concatenate([middle[:SPANS * SEGS - 2], jnp.array([0, REQS - 1], jnp.int32)]).astype(jnp.int32)
    order = jax.random.permutation(jax.random.fold_in(key, 32), SPANS * SEGS)
    return picked[order].reshape(SPANS, SEGS).astype(jnp.int32)


def level_of(rng, extent, split, smallest, top_value):
    level = 1.0
    for axis_at, parts in split:
        steps = jax.random.uniform(jax.random.fold_in(jax.random.fold_in(rng, 6), axis_at), (parts,), jnp.float32, smallest / len(split), top_value / len(split))
        level = level * jnp.repeat(jnp.exp(steps), extent[axis_at] // parts).reshape((-1,) + (1,) * (len(extent) - 1 - axis_at))
    return level


def split_up(number_of, total, limit, slope):
    weights = [(1 << 20) // math.isqrt(standing ** slope) + 1 for standing in range(2, number_of + 1)]
    rest, given = total - limit - (number_of - 1), [1] * (number_of - 1)
    while rest > 0:
        movable = [i for i in range(number_of - 1) if given[i] < limit]
        mass, budget = sum([weights[i] for i in movable]), rest
        for i in movable:
            more = min(limit - given[i], max(1, budget * weights[i] // mass), rest)
            given[i] = given[i] + more
            rest = rest - more
    return np.array([limit] + given)


def uneven(stream_key, count, total, reach, skew):
    if count == 2:
        one = jax.random.randint(stream_key, (), max(1, total - reach), min(reach, total - 1) + 1)
        return jnp.stack([one, total - one])
    lengths = jnp.asarray(split_up(count, total, reach, skew), jnp.int32)
    pairs = (count - 1) // 2
    giver, taker = lengths[1:1 + 2 * pairs:2], lengths[2:2 + 2 * pairs:2]
    room = jnp.minimum(giver - 1, reach - taker)
    passed = jax.random.randint(jax.random.fold_in(stream_key, 1), (pairs,), 0, 1 << 20) % (room + 1)
    lengths = lengths.at[1:1 + 2 * pairs:2].set(giver - passed).at[2:2 + 2 * pairs:2].set(taker + passed)
    return lengths[jax.random.permutation(jax.random.fold_in(stream_key, 2), count)]


def bell_draw(key, dims, deviation, most, split=(), kind=jnp.bfloat16):
    values = deviation * jax.random.normal(key, dims, jnp.float32)
    if split:
        values = values * level_of(key, dims, split, -0.22, 0.18)
    return jnp.clip(values, -most, most).astype(kind)


def setup_inputs(seed: int = 0, part: int = 0) -> dict:
    splits = jax.random.split(jax.random.key(seed), 11)
    part_keys = jax.random.split(jax.random.fold_in(splits[10], part), 11)
    latent_rows = draw_latent_rows(jax.random.fold_in(jax.random.fold_in(splits[10], part), 71), part)
    pre_queries = draw_pre_queries(jax.random.fold_in(jax.random.fold_in(splits[10], part), 71), part)
    pre_lengths = jax.vmap(lambda own: uneven(own, SEGS, PRE, PMOST, 1))(jax.random.split(part_keys[2], SPANS)).reshape((SPANS, SEGS)).astype(jnp.int32)
    owner_map = draw_owner_map(jax.random.fold_in(jax.random.fold_in(splits[10], part), 71), part)
    context_cache = bell_draw(part_keys[4], (REQS, CTX, KV), 1.0, 6.0, ((0, 16),))
    context_lengths = uneven(part_keys[5], REQS, REQS * CTX // 2, CTX, 2).astype(jnp.int32)
    new_latent = draw_new_latent(jax.random.fold_in(jax.random.fold_in(splits[10], part), 71), part)
    dec_queries = draw_dec_queries(jax.random.fold_in(jax.random.fold_in(splits[10], part), 71), part)
    key_weight = bell_draw(splits[8], (LAT, H * HD), LAT ** -0.5, 0.25, ((1, 8),))
    value_weight = bell_draw(splits[9], (LAT, H * HD), LAT ** -0.5, 0.25, ((1, 8),))
    return dict(latent_rows=latent_rows, pre_queries=pre_queries, pre_lengths=pre_lengths, owner_map=owner_map, context_cache=context_cache, context_lengths=context_lengths, new_latent=new_latent, dec_queries=dec_queries, key_weight=key_weight, value_weight=value_weight)


NEGATIVE = -1e+30

def request_table(pre_lengths, owner_map, span_len):
    seg_ends = jnp.cumsum(pre_lengths, axis=1)
    span_base = jnp.arange(pre_lengths.shape[0], dtype=jnp.int32)[:, None] * span_len
    seg_starts = seg_ends - pre_lengths + span_base
    return (owner_map.reshape(-1), seg_starts.reshape(-1), pre_lengths.reshape(-1))

def span_attention(span_rows, span_queries, span_lengths, key_weight, value_weight):
    score_scale = 1.0 / math.sqrt(HD + ROPE)
    seg_ends = jnp.cumsum(span_lengths)
    places = jnp.arange(PRE, dtype=jnp.int32)
    segment = lax.optimization_barrier(jnp.sum((places[:, None] >= seg_ends[None, :]).astype(jnp.int32), axis=1))
    allowed = (segment[:, None] == segment[None, :]) & (places[None, :] <= places[:, None])
    latent = span_rows[:, :LAT]
    rope_keys = span_rows[:, LAT:]

    def one_head(head_index):
        column = head_index * HD
        key_cols = lax.dynamic_slice_in_dim(key_weight, column, HD, 1)
        value_cols = lax.dynamic_slice_in_dim(value_weight, column, HD, 1)
        keys_nope = jnp.dot(latent, key_cols, preferred_element_type=jnp.float32).astype(jnp.bfloat16)
        values = jnp.dot(latent, value_cols, preferred_element_type=jnp.float32).astype(jnp.bfloat16)
        key_rows = jnp.concatenate([keys_nope, rope_keys], axis=1)
        queries = lax.dynamic_index_in_dim(span_queries, head_index, 1, keepdims=False)
        scores = jnp.dot(queries, key_rows.T, preferred_element_type=jnp.float32) * score_scale
        masked = jnp.where(allowed, scores, NEGATIVE)
        peak_score = lax.optimization_barrier(jnp.max(masked, axis=1, keepdims=True))
        weights = jnp.exp(masked - peak_score)
        weight_sum = lax.optimization_barrier(jnp.sum(weights, axis=1, keepdims=True))
        mixed_out = jnp.dot(weights.astype(jnp.bfloat16), values, preferred_element_type=jnp.float32) / weight_sum
        return mixed_out.astype(jnp.bfloat16)
    per_head = lax.map(one_head, jnp.arange(H, dtype=jnp.int32))
    return jnp.transpose(per_head, (1, 0, 2)).reshape(PRE, H * HD)

def reference(latent_rows, pre_queries, pre_lengths, owner_map, context_cache, context_lengths, new_latent, dec_queries, key_weight, value_weight):
    pieces = []
    for span in range(SPANS):
        pieces.append(span_attention(latent_rows[span * PRE:(span + 1) * PRE], pre_queries[span * PRE:(span + 1) * PRE], pre_lengths[span], key_weight, value_weight))
    prefill_out = jnp.concatenate(pieces, axis=0)
    flat_owner, flat_start, flat_length = request_table(pre_lengths, owner_map, PRE)
    row_ids = jnp.arange(REQS, dtype=jnp.int32)
    matches = (flat_owner[None, :] == row_ids[:, None]).astype(jnp.int32)
    is_target = lax.optimization_barrier(jnp.sum(matches, axis=1)) > 0
    first_row = lax.optimization_barrier(jnp.sum(matches * flat_start[None, :], axis=1)).astype(jnp.int32)
    prompt_len = lax.optimization_barrier(jnp.sum(matches * flat_length[None, :], axis=1))
    effective = jnp.where(is_target, prompt_len, context_lengths).astype(jnp.int32)
    padded = jnp.concatenate([latent_rows, jnp.zeros((PRE, KV), latent_rows.dtype)], axis=0)
    key_heads = key_weight.reshape(LAT, H, HD)
    value_heads = value_weight.reshape(LAT, H, HD)
    absorbed = jnp.einsum('srhd,lhd->srhl', dec_queries[..., :HD].astype(jnp.float32), key_heads.astype(jnp.float32)).astype(jnp.bfloat16)
    query_all = jnp.concatenate([absorbed, dec_queries[..., HD:]], axis=3)
    score_scale = 1.0 / math.sqrt(HD + ROPE)

    def one_row(entry):
        row_query, cache_rows, fresh_rows, row_length, row_target, row_first = entry
        replaced = lax.dynamic_slice_in_dim(padded, row_first, PRE, 0)
        front_rows = jnp.where(row_target, replaced, cache_rows[:PRE])
        key_rows = jnp.concatenate([front_rows, cache_rows[PRE:], fresh_rows], axis=0)
        flat_query = row_query.reshape(STEPS * H, KV)
        scores = jnp.dot(flat_query, key_rows.T, preferred_element_type=jnp.float32) * score_scale
        places = jnp.arange(CTX + STEPS, dtype=jnp.int32)
        step_of = jnp.arange(STEPS * H, dtype=jnp.int32) // H
        allowed = jnp.where(places[None, :] < CTX, places[None, :] < row_length, places[None, :] - CTX <= step_of[:, None])
        masked = jnp.where(allowed, scores, NEGATIVE)
        peak_score = lax.optimization_barrier(jnp.max(masked, axis=1, keepdims=True))
        weights = jnp.exp(masked - peak_score)
        weight_sum = lax.optimization_barrier(jnp.sum(weights, axis=1, keepdims=True))
        mixed_out = jnp.dot(weights.astype(jnp.bfloat16), key_rows[:, :LAT], preferred_element_type=jnp.float32) / weight_sum
        return mixed_out.astype(jnp.bfloat16).reshape(STEPS, H, LAT)
    latent_out = lax.map(one_row, (jnp.transpose(query_all, (1, 0, 2, 3)), context_cache, jnp.transpose(new_latent, (1, 0, 2)), effective, is_target, first_row))
    decode_out = jnp.einsum('rshl,lhd->srhd', latent_out.astype(jnp.float32), value_heads.astype(jnp.float32)).astype(jnp.bfloat16)
    return (prefill_out, decode_out.reshape(STEPS, REQS, H * HD))
```

```python
import functools
import math

import jax
import jax.numpy as jnp
from jax import lax
from jax.experimental import pallas as pl
from jax.experimental.pallas import tpu as pltpu
from jax.sharding import PartitionSpec as P

BLK = 512


NEGATIVE = -1e30


def from_partner(value, axis, distance):
    mask = 2**distance
    pairs = [(source, source ^ mask) for source in range(lax.axis_size(axis))]
    return lax.ppermute(value, axis, pairs)


def request_table(pre_lengths, owner_map, span_len):
    seg_ends = jnp.cumsum(pre_lengths, axis=1)
    span_base = jnp.arange(pre_lengths.shape[0], dtype=jnp.int32)[:, None] * span_len
    seg_starts = seg_ends - pre_lengths + span_base
    return (owner_map.reshape(-1), seg_starts.reshape(-1), pre_lengths.reshape(-1))


def prefill_heads(own_span, queries, span_lengths, key_weight, value_weight):
    span_len, head_count, query_width = queries.shape
    head_size = key_weight.shape[1] // head_count
    lat_width = key_weight.shape[0]
    score_scale = 1.0 / math.sqrt(query_width)
    latent = own_span[:, :lat_width]
    rope_keys = own_span[:, lat_width:]
    keys_nope = (
        jnp.dot(latent, key_weight, preferred_element_type=jnp.float32)
        .astype(jnp.bfloat16)
        .reshape(span_len, head_count, head_size)
    )
    values = (
        jnp.dot(latent, value_weight, preferred_element_type=jnp.float32)
        .astype(jnp.bfloat16)
        .reshape(span_len, head_count, head_size)
    )
    scores = jnp.einsum(
        "qhd,khd->hqk", queries[:, :, :head_size], keys_nope, preferred_element_type=jnp.float32
    )
    scores = scores + jnp.einsum(
        "qhr,kr->hqk", queries[:, :, head_size:], rope_keys, preferred_element_type=jnp.float32
    )
    scores = scores * score_scale
    seg_ends = jnp.cumsum(span_lengths)
    places = jnp.arange(span_len, dtype=jnp.int32)
    segment = jnp.sum((places[:, None] >= seg_ends[None, :]).astype(jnp.int32), axis=1)
    allowed = (segment[:, None] == segment[None, :]) & (places[None, :] <= places[:, None])
    masked = jnp.where(allowed[None], scores, NEGATIVE)
    peak_score = jnp.max(masked, axis=2, keepdims=True)
    weights = jnp.exp(masked - peak_score)
    weight_sum = jnp.sum(weights, axis=2)
    mixed_out = jnp.einsum(
        "hqk,khd->qhd", weights.astype(jnp.bfloat16), values, preferred_element_type=jnp.float32
    )
    mixed_out = mixed_out / jnp.transpose(weight_sum)[:, :, None]
    return mixed_out.astype(jnp.bfloat16).reshape(span_len, head_count * head_size)


def plain_on_device(
    latent_rows,
    pre_queries,
    pre_lengths,
    owner_map,
    context_cache,
    context_lengths,
    new_latent,
    dec_queries,
    key_weight,
    value_weight,
):
    head_rank = lax.axis_index("head")
    batch_rank = lax.axis_index("batch")
    span_len = pre_queries.shape[0]
    kv_width = latent_rows.shape[1]
    own_span = lax.all_gather(latent_rows, "head", axis=0, tiled=True)
    other_span = from_partner(own_span, "batch", 0)
    first_span = jnp.where(batch_rank == 0, own_span, other_span)
    second_span = jnp.where(batch_rank == 0, other_span, own_span)
    all_spans = jnp.concatenate([first_span, second_span], axis=0)
    span_lengths = lax.dynamic_index_in_dim(pre_lengths, batch_rank, 0, keepdims=False)
    prefill_out = prefill_heads(own_span, pre_queries, span_lengths, key_weight, value_weight)
    step_total, rows_local, head_count, query_width = dec_queries.shape
    lat_width = key_weight.shape[0]
    head_size = key_weight.shape[1] // head_count
    owned_rows = context_cache.shape[0]
    score_scale = 1.0 / math.sqrt(query_width)
    key_heads = key_weight.reshape(lat_width, head_count, head_size)
    value_heads = value_weight.reshape(lat_width, head_count, head_size)
    absorbed = jnp.einsum(
        "srhd,lhd->srhl",
        dec_queries[..., :head_size],
        key_heads,
        preferred_element_type=jnp.float32,
    ).astype(jnp.bfloat16)
    query_all = jnp.concatenate([absorbed, dec_queries[..., head_size:]], axis=3)
    flat_owner, flat_start, flat_length = request_table(pre_lengths, owner_map, span_len)
    row_ids = (
        batch_rank * rows_local + head_rank * owned_rows + jnp.arange(owned_rows, dtype=jnp.int32)
    )
    matches = (flat_owner[None, :] == row_ids[:, None]).astype(jnp.int32)
    is_target = jnp.sum(matches, axis=1) > 0
    first_row = jnp.sum(matches * flat_start[None, :], axis=1)
    prompt_len = jnp.sum(matches * flat_length[None, :], axis=1)
    effective = jnp.where(is_target, prompt_len, context_lengths)
    padded = jnp.concatenate([all_spans, jnp.zeros((span_len, kv_width), all_spans.dtype)], axis=0)
    replaced = jax.vmap(lambda offset: lax.dynamic_slice_in_dim(padded, offset, span_len, 0))(
        first_row
    )
    front_rows = jnp.where(is_target[:, None, None], replaced, context_cache[:, :span_len])
    front_blocks = span_len // BLK
    needed = (jnp.max(effective) + BLK - 1) // BLK
    fresh_latent = new_latent[..., :lat_width]
    owned_query = lax.all_to_all(query_all, "head", split_axis=1, concat_axis=2, tiled=True)
    fresh_scores = (
        jnp.einsum("srhk,jrk->srhj", owned_query, new_latent, preferred_element_type=jnp.float32)
        * score_scale
    )
    visible = (
        jnp.arange(new_latent.shape[0], dtype=jnp.int32)[None, :]
        <= jnp.arange(step_total, dtype=jnp.int32)[:, None]
    )
    fresh_scores = jnp.where(visible[:, None, None, :], fresh_scores, NEGATIVE)
    peak_score = jnp.max(fresh_scores, axis=3)
    weights = jnp.exp(fresh_scores - peak_score[..., None])
    weight_sum = jnp.sum(weights, axis=3)
    running = jnp.einsum(
        "srhj,jrl->srhl",
        weights.astype(jnp.bfloat16),
        fresh_latent,
        preferred_element_type=jnp.float32,
    )

    def advance(block_index, state_tuple, source):
        old_peak, old_sum, old_running = state_tuple
        key_block = lax.dynamic_slice_in_dim(source, block_index * BLK, BLK, 1)
        scores = (
            jnp.einsum("srhk,rtk->srht", owned_query, key_block, preferred_element_type=jnp.float32)
            * score_scale
        )
        places = block_index * BLK + jnp.arange(BLK, dtype=jnp.int32)
        in_context = places[None, :] < effective[:, None]
        scores = jnp.where(in_context[None, :, None, :], scores, NEGATIVE)
        new_peak = jnp.maximum(old_peak, jnp.max(scores, axis=3))
        factor = jnp.exp(old_peak - new_peak)
        block_weights = jnp.exp(scores - new_peak[..., None])
        new_sum = old_sum * factor + jnp.sum(block_weights, axis=3)
        new_running = old_running * factor[..., None] + jnp.einsum(
            "srht,rtl->srhl",
            block_weights.astype(jnp.bfloat16),
            key_block[..., :lat_width],
            preferred_element_type=jnp.float32,
        )
        return (new_peak, new_sum, new_running)

    state_tuple = lax.fori_loop(
        0,
        jnp.minimum(needed, front_blocks),
        lambda block_index, state_now: advance(block_index, state_now, front_rows),
        (peak_score, weight_sum, running),
    )
    state_tuple = lax.fori_loop(
        front_blocks,
        jnp.maximum(needed, front_blocks),
        lambda block_index, state_now: advance(block_index, state_now, context_cache),
        state_tuple,
    )
    latent_out = (state_tuple[2] / state_tuple[1][..., None]).astype(jnp.bfloat16)
    returned = lax.all_to_all(latent_out, "head", split_axis=2, concat_axis=1, tiled=True)
    projected = jnp.einsum(
        "srhl,lhd->srhd", returned, value_heads, preferred_element_type=jnp.float32
    ).astype(jnp.bfloat16)
    decode_out = projected.reshape(query_all.shape[0], rows_local, head_count * head_size)
    return (prefill_out, decode_out)


def trans_dot(left, right):
    return lax.dot_general(
        left, right, (((1,), (1,)), ((), ())), preferred_element_type=jnp.float32
    )


def prefill_kernel(
    lens_ref, latent_ref, q_ref, kw_ref, vw_ref, out_ref, bias_ref, keys_ref, vals_ref, *, lat, qb, look, scale
):
    span_len = latent_ref.shape[0]
    pair = keys_ref.shape[0]
    segs = lens_ref.shape[0]
    blocks = span_len // qb
    ends = []
    total = 0
    for k in range(segs):
        total = total + lens_ref[k]
        ends.append(total)

    @pl.when(pl.program_id(0) == 0)
    def _():
        rope = latent_ref[:, lat:]
        for p in range(pair):
            keys_ref[p, :, 128:] = jnp.concatenate([rope, jnp.zeros_like(rope)], axis=1)
        width = (look + 1) * qb
        for i in range(blocks):
            rows = i * qb + lax.broadcasted_iota(jnp.int32, (qb, width), 0)
            cols = (i - look) * qb + lax.broadcasted_iota(jnp.int32, (qb, width), 1)
            row_start = jnp.zeros((qb, width), jnp.int32)
            for end in ends:
                row_start = jnp.where(rows >= end, end, row_start)
            seen = (cols >= row_start) & (cols <= rows)
            bias_ref[i] = jnp.where(seen, 0.0, NEGATIVE)

    latent = latent_ref[:, :lat]
    keys = jnp.dot(latent, kw_ref[...], preferred_element_type=jnp.float32).astype(jnp.bfloat16)
    for p in range(pair):
        keys_ref[p, :, :128] = keys[:, p * 128 : (p + 1) * 128]
    vals_ref[...] = jnp.dot(latent, vw_ref[...], preferred_element_type=jnp.float32).astype(
        jnp.bfloat16
    )

    def attend(i, back):
        lo, hi = (i - back) * qb, (i + 1) * qb
        bias = bias_ref[i, :, (look - back) * qb :]
        for p in range(pair):
            s = trans_dot(q_ref[p, i * qb : hi, :], keys_ref[p, lo:hi, :]) + bias
            m = jnp.max(s, axis=1, keepdims=True)
            w = jnp.exp2((s - m) * scale)
            l = jnp.sum(w, axis=1, keepdims=True)
            o = jnp.dot(
                w.astype(jnp.bfloat16),
                vals_ref[lo:hi, p * 128 : (p + 1) * 128],
                preferred_element_type=jnp.float32,
            )
            out_ref[i * qb : hi, p * 128 : (p + 1) * 128] = (o / l).astype(out_ref.dtype)

    for i in range(blocks):
        most = min(i, look)
        if most == 0:
            attend(i, 0)
            continue
        first = jnp.int32(0)
        for end in ends:
            first = jnp.where(i * qb >= end, end, first)
        need = i - first // qb
        for back in range(most + 1):
            pl.when(need == back)(functools.partial(attend, i, back))


def prefill_pallas(own_span, queries, span_lengths, key_weight, value_weight, qb=256):
    span_len, heads, width = queries.shape
    lat = key_weight.shape[0]
    kv = own_span.shape[1]
    most_request = span_len // 2
    look = min(-(-most_request // qb), span_len // qb - 1)
    pair = 2
    scale = math.log2(math.e) / math.sqrt(width)
    q_pad = jnp.pad(jnp.transpose(queries, (1, 0, 2)), ((0, 0), (0, 0), (0, 256 - width)))
    return pl.pallas_call(
        functools.partial(prefill_kernel, lat=lat, qb=qb, look=look, scale=scale),
        out_shape=jax.ShapeDtypeStruct((span_len, heads * 128), jnp.bfloat16),
        grid_spec=pltpu.PrefetchScalarGridSpec(
            num_scalar_prefetch=1,
            grid=(heads // pair,),
            in_specs=[
                pl.BlockSpec((span_len, kv), lambda g, _: (0, 0)),
                pl.BlockSpec((pair, span_len, 256), lambda g, _: (g, 0, 0)),
                pl.BlockSpec((lat, pair * 128), lambda g, _: (0, g)),
                pl.BlockSpec((lat, pair * 128), lambda g, _: (0, g)),
            ],
            out_specs=pl.BlockSpec((span_len, pair * 128), lambda g, _: (0, g)),
            scratch_shapes=[
                pltpu.VMEM((span_len // qb, qb, (look + 1) * qb), jnp.float32),
                pltpu.VMEM((pair, span_len, 256), jnp.bfloat16),
                pltpu.VMEM((span_len, pair * 128), jnp.bfloat16),
            ],
        ),
        compiler_params=pltpu.CompilerParams(
            dimension_semantics=("arbitrary",), vmem_limit_bytes=40 << 20
        ),
        cost_estimate=pl.CostEstimate(
            flops=12 * 10**9, bytes_accessed=20 << 20, transcendentals=8 << 20
        ),
    )(span_lengths, own_span, q_pad, key_weight, value_weight)


def decode_kernel(
    info_ref, q_ref, fresh_ref, spans_ref, cache_ref, out_ref, bufs, sems, m_ref, l_ref, acc_ref, *, lat, heads, blk, depth, scale
):
    owned = q_ref.shape[0]
    rows = q_ref.shape[1]

    def copy_of(r, t):
        slot = lax.rem(t, depth)
        place = info_ref[1, r] // blk * blk + t * blk
        place = pl.multiple_of(place, blk)

        @pl.when(info_ref[0, r] > 0)
        def _():
            pltpu.make_async_copy(
                spans_ref.at[pl.ds(place, blk)], bufs.at[r, slot], sems.at[r, slot]
            ).start()

        @pl.when(info_ref[0, r] == 0)
        def _():
            pltpu.make_async_copy(
                cache_ref.at[r, pl.ds(place, blk)], bufs.at[r, slot], sems.at[r, slot]
            ).start()

    counts = []
    for r in range(owned):
        start, length = info_ref[1, r], info_ref[2, r]
        counts.append((start + length + blk - 1) // blk - start // blk)
    for r in range(owned):
        for t in range(depth - 1):
            pl.when(t < counts[r])(functools.partial(copy_of, r, jnp.int32(t)))
    for r in range(owned):
        start, length = info_ref[1, r], info_ref[2, r]
        base = start // blk * blk
        q = q_ref[r]
        fresh = fresh_ref[r]
        s = trans_dot(q, fresh)
        row_step = (lax.broadcasted_iota(jnp.int32, s.shape, 0) // heads) % 2
        col = lax.broadcasted_iota(jnp.int32, s.shape, 1)
        s = jnp.where(col <= row_step, s, NEGATIVE)
        m = jnp.max(s, axis=1, keepdims=True)
        w = jnp.exp2((s - m) * scale)
        l_ref[...] = jnp.broadcast_to(jnp.sum(w, axis=1, keepdims=True), l_ref.shape)
        m_ref[...] = jnp.broadcast_to(m, m_ref.shape)
        acc_ref[...] = jnp.dot(
            w.astype(jnp.bfloat16), fresh[:, :lat], preferred_element_type=jnp.float32
        )

        def step(t, carry):
            slot = lax.rem(t, depth)
            pl.when(t + depth - 1 < counts[r])(lambda: copy_of(r, t + depth - 1))
            pltpu.make_async_copy(
                cache_ref.at[r, pl.ds(0, blk)], bufs.at[r, slot], sems.at[r, slot]
            ).wait()
            keys = bufs[r, slot]
            s = trans_dot(q, keys)
            place = base + t * blk + lax.broadcasted_iota(jnp.int32, (1, blk), 1)
            hide = jnp.where((place >= start) & (place < start + length), 0.0, NEGATIVE)
            s = s + hide
            old = m_ref[:, :1]
            new = jnp.maximum(old, jnp.max(s, axis=1, keepdims=True))
            alpha = jnp.exp2((old - new) * scale)
            w = jnp.exp2((s - new) * scale)
            l_new = l_ref[:, :1] * alpha + jnp.sum(w, axis=1, keepdims=True)
            l_ref[...] = jnp.broadcast_to(l_new, l_ref.shape)
            m_ref[...] = jnp.broadcast_to(new, m_ref.shape)
            acc_ref[...] = acc_ref[...] * alpha + jnp.dot(
                w.astype(jnp.bfloat16), keys[:, :lat], preferred_element_type=jnp.float32
            )
            return carry

        lax.fori_loop(0, counts[r], step, 0)
        out_ref[r] = (acc_ref[...] / l_ref[:, :1]).astype(out_ref.dtype)


def decode_pallas(info, query, fresh, spans, cache, lat, heads, width, blk=512, depth=4):
    owned, rows, kv = query.shape
    return pl.pallas_call(
        functools.partial(
            decode_kernel,
            lat=lat,
            heads=heads,
            blk=blk,
            depth=depth,
            scale=math.log2(math.e) / math.sqrt(width),
        ),
        out_shape=jax.ShapeDtypeStruct((owned, rows, lat), jnp.bfloat16),
        in_specs=[
            pl.BlockSpec(memory_space=pltpu.SMEM),
            pl.BlockSpec(memory_space=pltpu.VMEM),
            pl.BlockSpec(memory_space=pltpu.VMEM),
            pl.BlockSpec(memory_space=pl.ANY),
            pl.BlockSpec(memory_space=pl.ANY),
        ],
        out_specs=pl.BlockSpec(memory_space=pltpu.VMEM),
        scratch_shapes=[
            pltpu.VMEM((owned, depth, blk, kv), jnp.bfloat16),
            pltpu.SemaphoreType.DMA((owned, depth)),
            pltpu.VMEM((rows, 128), jnp.float32),
            pltpu.VMEM((rows, 128), jnp.float32),
            pltpu.VMEM((rows, lat), jnp.float32),
        ],
        compiler_params=pltpu.CompilerParams(vmem_limit_bytes=40 << 20),
        cost_estimate=pl.CostEstimate(
            flops=5 * 10**9, bytes_accessed=10 << 20, transcendentals=2 << 20
        ),
    )(info, query, fresh, spans, cache)


def absorb_into(dq_ref, kw_ref, out_ref, flat, wide, heads, lat, step):
    rows = dq_ref.shape[0]
    flat[...] = dq_ref[:, :128].astype(jnp.float32)
    count = rows // heads
    for h in range(heads):
        mine = flat[pl.ds(h, count, stride=heads), :].astype(jnp.bfloat16)
        res = trans_dot(mine, kw_ref[:, h * 128 : (h + 1) * 128])
        for c in range(lat // 128):
            wide[c, pl.ds(h, count, stride=heads), :] = res[:, c * 128 : (c + 1) * 128]
    for c in range(lat // 128):
        out_ref[:, c * 128 : (c + 1) * 128] = wide[c].astype(jnp.bfloat16)
    out_ref[:, lat:] = dq_ref[:, 128:]


def absorb_kernel(dq_ref, kw_ref, out_ref, flat, wide, *, heads, lat):
    absorb_into(dq_ref, kw_ref, out_ref, flat, wide, heads, lat, 1)


def absorb_pallas(flat_queries, key_weight, heads):
    rows, width = flat_queries.shape
    lat = key_weight.shape[0]
    vm = pl.BlockSpec(memory_space=pltpu.VMEM)
    return pl.pallas_call(
        functools.partial(absorb_kernel, heads=heads, lat=lat),
        out_shape=jax.ShapeDtypeStruct((rows, lat + width - 128), jnp.bfloat16),
        in_specs=[vm, vm],
        out_specs=vm,
        scratch_shapes=[
            pltpu.VMEM((rows, 128), jnp.float32),
            pltpu.VMEM((lat // 128, rows, 128), jnp.float32),
        ],
        compiler_params=pltpu.CompilerParams(vmem_limit_bytes=24 << 20),
    )(flat_queries, key_weight)


def project_into(x_ref, vw_ref, out_ref, wide, heads, lat):
    rows = x_ref.shape[0]
    count = rows // heads
    for c in range(lat // 128):
        wide[c] = x_ref[:, c * 128 : (c + 1) * 128].astype(jnp.float32)
    for h in range(heads):
        mine = jnp.concatenate(
            [wide[c, pl.ds(h, count, stride=heads), :] for c in range(lat // 128)], axis=1
        ).astype(jnp.bfloat16)
        out_ref[:, h * 128 : (h + 1) * 128] = jnp.dot(
            mine, vw_ref[:, h * 128 : (h + 1) * 128], preferred_element_type=jnp.float32
        ).astype(jnp.bfloat16)


def project_kernel(x_ref, vw_ref, out_ref, wide, *, heads, lat):
    project_into(x_ref, vw_ref, out_ref, wide, heads, lat)


def project_pallas(flat_latent, value_weight, heads):
    rows, lat = flat_latent.shape
    vm = pl.BlockSpec(memory_space=pltpu.VMEM)
    return pl.pallas_call(
        functools.partial(project_kernel, heads=heads, lat=lat),
        out_shape=jax.ShapeDtypeStruct((rows // heads, heads * 128), jnp.bfloat16),
        in_specs=[vm, vm],
        out_specs=vm,
        scratch_shapes=[pltpu.VMEM((lat // 128, rows, 128), jnp.float32)],
        compiler_params=pltpu.CompilerParams(vmem_limit_bytes=24 << 20),
    )(flat_latent, value_weight)


def on_device(
    latent_rows,
    pre_queries,
    pre_lengths,
    owner_map,
    context_cache,
    context_lengths,
    new_latent,
    dec_queries,
    key_weight,
    value_weight,
):
    steps, rows_local, heads, width = dec_queries.shape
    if heads % 16 or latent_rows.shape[0] % 16:
        return plain_on_device(
            latent_rows,
            pre_queries,
            pre_lengths,
            owner_map,
            context_cache,
            context_lengths,
            new_latent,
            dec_queries,
            key_weight,
            value_weight,
        )
    head_rank = lax.axis_index("head")
    batch_rank = lax.axis_index("batch")
    ranks = lax.axis_size("head")
    span_len = pre_queries.shape[0]
    kv = latent_rows.shape[1]
    lat = key_weight.shape[0]
    owned = context_cache.shape[0]
    span_lengths = lax.dynamic_index_in_dim(pre_lengths, batch_rank, 0, keepdims=False)
    flat_owner, flat_start, flat_length = request_table(pre_lengths, owner_map, span_len)
    row_ids = batch_rank * rows_local + head_rank * owned + jnp.arange(owned, dtype=jnp.int32)
    matches = (flat_owner[None, :] == row_ids[:, None]).astype(jnp.int32)
    is_target = jnp.sum(matches, axis=1)
    first_row = jnp.sum(matches * flat_start[None, :], axis=1)
    prompt_len = jnp.sum(matches * flat_length[None, :], axis=1)
    effective = jnp.where(is_target > 0, prompt_len, context_lengths)
    info = jnp.stack([is_target, first_row, effective])
    fresh = jnp.pad(
        jnp.transpose(new_latent, (1, 0, 2)), ((0, 0), (0, 128 - steps), (0, 0))
    )
    absorbed = absorb_pallas(dec_queries.reshape(-1, width), key_weight, heads)
    query_all = absorbed.reshape(steps, rows_local, heads, kv)
    own_span = lax.all_gather(latent_rows, "head", axis=0, tiled=True)
    other_span = from_partner(own_span, "batch", 0)
    first_span = jnp.where(batch_rank == 0, own_span, other_span)
    second_span = jnp.where(batch_rank == 0, other_span, own_span)
    all_spans = jnp.concatenate([first_span, second_span], axis=0)
    got = lax.all_to_all(query_all, "head", split_axis=1, concat_axis=2, tiled=True)
    query = jnp.transpose(got, (1, 0, 2, 3)).reshape(owned, steps * ranks * heads, kv)
    latent_out = decode_pallas(
        info, query, fresh, all_spans, context_cache, lat, ranks * heads, width
    )
    back = jnp.transpose(latent_out.reshape(owned, steps, ranks * heads, lat), (1, 0, 2, 3))
    returned = lax.all_to_all(back, "head", split_axis=2, concat_axis=1, tiled=True)
    prefill_out = prefill_pallas(own_span, pre_queries, span_lengths, key_weight, value_weight)
    decode_out = project_pallas(returned.reshape(-1, lat), value_weight, heads)
    return (prefill_out, decode_out.reshape(steps, rows_local, heads * 128))


def solution(mesh):
    placed = (
        P(("groups", "batch", "head"), None),
        P(("groups", "batch"), "head", None),
        P("groups", None),
        P("groups", None),
        P(("groups", "batch", "head"), None, None),
        P(("groups", "batch", "head")),
        P("groups", ("batch", "head"), None),
        P("groups", "batch", "head", None),
        P(None, "head"),
        P(None, "head"),
    )
    return jax.shard_map(
        on_device,
        mesh=mesh,
        in_specs=placed,
        out_specs=(P(("groups", "batch"), "head"), P("groups", "batch", "head")),
        check_vma=False,
    )
```

```python
import functools
import math

import jax
import jax.numpy as jnp
from jax import lax
from jax.experimental import pallas as pl
from jax.experimental.pallas import tpu as pltpu
from jax.sharding import PartitionSpec as P

BLK = 512


NEGATIVE = -1e30


def from_partner(value, axis, distance):
    mask = 2**distance
    pairs = [(source, source ^ mask) for source in range(lax.axis_size(axis))]
    return lax.ppermute(value, axis, pairs)


def request_table(pre_lengths, owner_map, span_len):
    seg_ends = jnp.cumsum(pre_lengths, axis=1)
    span_base = jnp.arange(pre_lengths.shape[0], dtype=jnp.int32)[:, None] * span_len
    seg_starts = seg_ends - pre_lengths + span_base
    return (owner_map.reshape(-1), seg_starts.reshape(-1), pre_lengths.reshape(-1))


def prefill_heads(own_span, queries, span_lengths, key_weight, value_weight):
    span_len, head_count, query_width = queries.shape
    head_size = key_weight.shape[1] // head_count
    lat_width = key_weight.shape[0]
    score_scale = 1.0 / math.sqrt(query_width)
    latent = own_span[:, :lat_width]
    rope_keys = own_span[:, lat_width:]
    keys_nope = (
        jnp.dot(latent, key_weight, preferred_element_type=jnp.float32)
        .astype(jnp.bfloat16)
        .reshape(span_len, head_count, head_size)
    )
    values = (
        jnp.dot(latent, value_weight, preferred_element_type=jnp.float32)
        .astype(jnp.bfloat16)
        .reshape(span_len, head_count, head_size)
    )
    scores = jnp.einsum(
        "qhd,khd->hqk", queries[:, :, :head_size], keys_nope, preferred_element_type=jnp.float32
    )
    scores = scores + jnp.einsum(
        "qhr,kr->hqk", queries[:, :, head_size:], rope_keys, preferred_element_type=jnp.float32
    )
    scores = scores * score_scale
    seg_ends = jnp.cumsum(span_lengths)
    places = jnp.arange(span_len, dtype=jnp.int32)
    segment = jnp.sum((places[:, None] >= seg_ends[None, :]).astype(jnp.int32), axis=1)
    allowed = (segment[:, None] == segment[None, :]) & (places[None, :] <= places[:, None])
    masked = jnp.where(allowed[None], scores, NEGATIVE)
    peak_score = jnp.max(masked, axis=2, keepdims=True)
    weights = jnp.exp(masked - peak_score)
    weight_sum = jnp.sum(weights, axis=2)
    mixed_out = jnp.einsum(
        "hqk,khd->qhd", weights.astype(jnp.bfloat16), values, preferred_element_type=jnp.float32
    )
    mixed_out = mixed_out / jnp.transpose(weight_sum)[:, :, None]
    return mixed_out.astype(jnp.bfloat16).reshape(span_len, head_count * head_size)


def plain_on_device(
    latent_rows,
    pre_queries,
    pre_lengths,
    owner_map,
    context_cache,
    context_lengths,
    new_latent,
    dec_queries,
    key_weight,
    value_weight,
):
    head_rank = lax.axis_index("head")
    batch_rank = lax.axis_index("batch")
    span_len = pre_queries.shape[0]
    kv_width = latent_rows.shape[1]
    own_span = lax.all_gather(latent_rows, "head", axis=0, tiled=True)
    other_span = from_partner(own_span, "batch", 0)
    first_span = jnp.where(batch_rank == 0, own_span, other_span)
    second_span = jnp.where(batch_rank == 0, other_span, own_span)
    all_spans = jnp.concatenate([first_span, second_span], axis=0)
    span_lengths = lax.dynamic_index_in_dim(pre_lengths, batch_rank, 0, keepdims=False)
    prefill_out = prefill_heads(own_span, pre_queries, span_lengths, key_weight, value_weight)
    step_total, rows_local, head_count, query_width = dec_queries.shape
    lat_width = key_weight.shape[0]
    head_size = key_weight.shape[1] // head_count
    owned_rows = context_cache.shape[0]
    score_scale = 1.0 / math.sqrt(query_width)
    key_heads = key_weight.reshape(lat_width, head_count, head_size)
    value_heads = value_weight.reshape(lat_width, head_count, head_size)
    absorbed = jnp.einsum(
        "srhd,lhd->srhl",
        dec_queries[..., :head_size],
        key_heads,
        preferred_element_type=jnp.float32,
    ).astype(jnp.bfloat16)
    query_all = jnp.concatenate([absorbed, dec_queries[..., head_size:]], axis=3)
    flat_owner, flat_start, flat_length = request_table(pre_lengths, owner_map, span_len)
    row_ids = (
        batch_rank * rows_local + head_rank * owned_rows + jnp.arange(owned_rows, dtype=jnp.int32)
    )
    matches = (flat_owner[None, :] == row_ids[:, None]).astype(jnp.int32)
    is_target = jnp.sum(matches, axis=1) > 0
    first_row = jnp.sum(matches * flat_start[None, :], axis=1)
    prompt_len = jnp.sum(matches * flat_length[None, :], axis=1)
    effective = jnp.where(is_target, prompt_len, context_lengths)
    padded = jnp.concatenate([all_spans, jnp.zeros((span_len, kv_width), all_spans.dtype)], axis=0)
    replaced = jax.vmap(lambda offset: lax.dynamic_slice_in_dim(padded, offset, span_len, 0))(
        first_row
    )
    front_rows = jnp.where(is_target[:, None, None], replaced, context_cache[:, :span_len])
    front_blocks = span_len // BLK
    needed = (jnp.max(effective) + BLK - 1) // BLK
    fresh_latent = new_latent[..., :lat_width]
    owned_query = lax.all_to_all(query_all, "head", split_axis=1, concat_axis=2, tiled=True)
    fresh_scores = (
        jnp.einsum("srhk,jrk->srhj", owned_query, new_latent, preferred_element_type=jnp.float32)
        * score_scale
    )
    visible = (
        jnp.arange(new_latent.shape[0], dtype=jnp.int32)[None, :]
        <= jnp.arange(step_total, dtype=jnp.int32)[:, None]
    )
    fresh_scores = jnp.where(visible[:, None, None, :], fresh_scores, NEGATIVE)
    peak_score = jnp.max(fresh_scores, axis=3)
    weights = jnp.exp(fresh_scores - peak_score[..., None])
    weight_sum = jnp.sum(weights, axis=3)
    running = jnp.einsum(
        "srhj,jrl->srhl",
        weights.astype(jnp.bfloat16),
        fresh_latent,
        preferred_element_type=jnp.float32,
    )

    def advance(block_index, state_tuple, source):
        old_peak, old_sum, old_running = state_tuple
        key_block = lax.dynamic_slice_in_dim(source, block_index * BLK, BLK, 1)
        scores = (
            jnp.einsum("srhk,rtk->srht", owned_query, key_block, preferred_element_type=jnp.float32)
            * score_scale
        )
        places = block_index * BLK + jnp.arange(BLK, dtype=jnp.int32)
        in_context = places[None, :] < effective[:, None]
        scores = jnp.where(in_context[None, :, None, :], scores, NEGATIVE)
        new_peak = jnp.maximum(old_peak, jnp.max(scores, axis=3))
        factor = jnp.exp(old_peak - new_peak)
        block_weights = jnp.exp(scores - new_peak[..., None])
        new_sum = old_sum * factor + jnp.sum(block_weights, axis=3)
        new_running = old_running * factor[..., None] + jnp.einsum(
            "srht,rtl->srhl",
            block_weights.astype(jnp.bfloat16),
            key_block[..., :lat_width],
            preferred_element_type=jnp.float32,
        )
        return (new_peak, new_sum, new_running)

    state_tuple = lax.fori_loop(
        0,
        jnp.minimum(needed, front_blocks),
        lambda block_index, state_now: advance(block_index, state_now, front_rows),
        (peak_score, weight_sum, running),
    )
    state_tuple = lax.fori_loop(
        front_blocks,
        jnp.maximum(needed, front_blocks),
        lambda block_index, state_now: advance(block_index, state_now, context_cache),
        state_tuple,
    )
    latent_out = (state_tuple[2] / state_tuple[1][..., None]).astype(jnp.bfloat16)
    returned = lax.all_to_all(latent_out, "head", split_axis=2, concat_axis=1, tiled=True)
    projected = jnp.einsum(
        "srhl,lhd->srhd", returned, value_heads, preferred_element_type=jnp.float32
    ).astype(jnp.bfloat16)
    decode_out = projected.reshape(query_all.shape[0], rows_local, head_count * head_size)
    return (prefill_out, decode_out)


def trans_dot(left, right):
    return lax.dot_general(
        left, right, (((1,), (1,)), ((), ())), preferred_element_type=jnp.float32
    )


def prefill_kernel(
    lens_ref, shards_ref, q_ref, kw_ref, vw_ref, out_ref, bias_ref, keys_ref, vals_ref, latent_ref, *, lat, qb, look, scale
):
    span_len = latent_ref.shape[0]
    own = shards_ref.shape[2]
    pair = keys_ref.shape[0]
    segs = lens_ref.shape[0]
    blocks = span_len // qb
    ends = []
    total = 0
    for k in range(segs):
        total = total + lens_ref[k]
        ends.append(total)

    @pl.when(pl.program_id(0) == 0)
    def _():
        for k in range(span_len // own):
            latent_ref[k * own : (k + 1) * own, :] = jnp.transpose(shards_ref[k])
        for p in range(pair):
            keys_ref[p, :, 128:] = latent_ref[:, lat:]
        width = (look + 1) * qb
        for i in range(blocks):
            rows = i * qb + lax.broadcasted_iota(jnp.int32, (width, qb), 1)
            cols = (i - look) * qb + lax.broadcasted_iota(jnp.int32, (width, qb), 0)
            row_start = jnp.zeros((width, qb), jnp.int32)
            for end in ends:
                row_start = jnp.where(rows >= end, end, row_start)
            seen = (cols >= row_start) & (cols <= rows)
            bias_ref[i] = jnp.where(seen, 0.0, NEGATIVE)

    latent = latent_ref[:, :lat]
    keys = jnp.dot(latent, kw_ref[...], preferred_element_type=jnp.float32).astype(jnp.bfloat16)
    for p in range(pair):
        keys_ref[p, :, :128] = keys[:, p * 128 : (p + 1) * 128]
    vals = jnp.dot(latent, vw_ref[...], preferred_element_type=jnp.float32)
    vals_ref[...] = jnp.transpose(vals.astype(jnp.bfloat16))

    def attend(i, back):
        lo, hi = (i - back) * qb, (i + 1) * qb
        bias = bias_ref[i, (look - back) * qb :, :]
        for p in range(pair):
            s = (
                jnp.dot(
                    keys_ref[p, lo:hi, :],
                    q_ref[p, :, i * qb : hi],
                    preferred_element_type=jnp.float32,
                )
                + bias
            )
            m = jnp.max(s, axis=0, keepdims=True)
            w = jnp.exp2((s - m) * scale)
            l = jnp.sum(w, axis=0, keepdims=True)
            o = jnp.dot(
                vals_ref[p * 128 : (p + 1) * 128, lo:hi],
                w.astype(jnp.bfloat16),
                preferred_element_type=jnp.float32,
            )
            o = jnp.transpose(o / l)
            out_ref[i * qb : hi, p * 128 : (p + 1) * 128] = o.astype(out_ref.dtype)

    for i in range(blocks):
        most = min(i, look)
        if most == 0:
            attend(i, 0)
            continue
        first = jnp.int32(0)
        for end in ends:
            first = jnp.where(i * qb >= end, end, first)
        need = i - first // qb
        for back in range(most + 1):
            pl.when(need == back)(functools.partial(attend, i, back))


def prefill_pallas(own_span, queries, span_lengths, key_weight, value_weight, qb=256):
    span_len, heads, width = queries.shape
    lat = key_weight.shape[0]
    kv = own_span.shape[1]
    shards, _, own = own_span.shape
    most_request = span_len // 2
    look = min(-(-most_request // qb), span_len // qb - 1)
    pair = 2
    scale = math.log2(math.e) / math.sqrt(width)
    q_turned = jnp.transpose(queries, (1, 2, 0))
    return pl.pallas_call(
        functools.partial(prefill_kernel, lat=lat, qb=qb, look=look, scale=scale),
        out_shape=jax.ShapeDtypeStruct((span_len, heads * 128), jnp.bfloat16),
        grid_spec=pltpu.PrefetchScalarGridSpec(
            num_scalar_prefetch=1,
            grid=(heads // pair,),
            in_specs=[
                pl.BlockSpec((shards, kv, own), lambda g, _: (0, 0, 0)),
                pl.BlockSpec((pair, width, span_len), lambda g, _: (g, 0, 0)),
                pl.BlockSpec((lat, pair * 128), lambda g, _: (0, g)),
                pl.BlockSpec((lat, pair * 128), lambda g, _: (0, g)),
            ],
            out_specs=pl.BlockSpec((span_len, pair * 128), lambda g, _: (0, g)),
            scratch_shapes=[
                pltpu.VMEM((span_len // qb, (look + 1) * qb, qb), jnp.float32),
                pltpu.VMEM((pair, span_len, width), jnp.bfloat16),
                pltpu.VMEM((pair * 128, span_len), jnp.bfloat16),
                pltpu.VMEM((span_len, kv), jnp.bfloat16),
            ],
        ),
        compiler_params=pltpu.CompilerParams(
            dimension_semantics=("arbitrary",), vmem_limit_bytes=40 << 20
        ),
        cost_estimate=pl.CostEstimate(
            flops=12 * 10**9, bytes_accessed=20 << 20, transcendentals=8 << 20
        ),
    )(span_lengths, own_span, q_turned, key_weight, value_weight)


def decode_kernel(
    info_ref, q_ref, fresh_ref, spans_ref, cache_ref, out_ref, bufs, sems, m_ref, l_ref, acc_ref, *, lat, heads, blk, depth, scale
):
    owned = q_ref.shape[0]
    rows = q_ref.shape[1]

    def copy_of(r, t):
        slot = lax.rem(t, depth)
        place = info_ref[1, r] // blk * blk + t * blk
        place = pl.multiple_of(place, blk)

        @pl.when(info_ref[0, r] > 0)
        def _():
            own = spans_ref.shape[2]
            for c in range(blk // own):
                pltpu.make_async_copy(
                    spans_ref.at[place // own + c],
                    bufs.at[r, slot, :, c * own : (c + 1) * own],
                    sems.at[r, slot],
                ).start()

        @pl.when(info_ref[0, r] == 0)
        def _():
            pltpu.make_async_copy(
                cache_ref.at[r, :, pl.ds(place, blk)], bufs.at[r, slot], sems.at[r, slot]
            ).start()

    counts = []
    for r in range(owned):
        start, length = info_ref[1, r], info_ref[2, r]
        counts.append((start + length + blk - 1) // blk - start // blk)
    for r in range(owned):
        for t in range(depth - 1):
            pl.when(t < counts[r])(functools.partial(copy_of, r, jnp.int32(t)))
    for r in range(owned):
        start, length = info_ref[1, r], info_ref[2, r]
        base = start // blk * blk
        q = q_ref[r]
        fresh = fresh_ref[r]
        s = trans_dot(q, fresh)
        row_step = (lax.broadcasted_iota(jnp.int32, s.shape, 0) // heads) % 2
        col = lax.broadcasted_iota(jnp.int32, s.shape, 1)
        s = jnp.where(col <= row_step, s, NEGATIVE)
        m = jnp.max(s, axis=1, keepdims=True)
        w = jnp.exp2((s - m) * scale)
        l_ref[...] = jnp.broadcast_to(jnp.sum(w, axis=1, keepdims=True), l_ref.shape)
        m_ref[...] = jnp.broadcast_to(m, m_ref.shape)
        acc_ref[...] = jnp.dot(
            w.astype(jnp.bfloat16), fresh[:, :lat], preferred_element_type=jnp.float32
        )

        def step(t, carry):
            slot = lax.rem(t, depth)
            pl.when(t + depth - 1 < counts[r])(lambda: copy_of(r, t + depth - 1))
            pltpu.make_async_copy(
                cache_ref.at[r, :, pl.ds(0, blk)], bufs.at[r, slot], sems.at[r, slot]
            ).wait()
            keys = bufs[r, slot]
            s = jnp.dot(q, keys, preferred_element_type=jnp.float32)
            place = base + t * blk + lax.broadcasted_iota(jnp.int32, (1, blk), 1)
            hide = jnp.where((place >= start) & (place < start + length), 0.0, NEGATIVE)
            s = s + hide
            old = m_ref[:, :1]
            new = jnp.maximum(old, jnp.max(s, axis=1, keepdims=True))
            alpha = jnp.exp2((old - new) * scale)
            w = jnp.exp2((s - new) * scale)
            l_new = l_ref[:, :1] * alpha + jnp.sum(w, axis=1, keepdims=True)
            l_ref[...] = jnp.broadcast_to(l_new, l_ref.shape)
            m_ref[...] = jnp.broadcast_to(new, m_ref.shape)
            acc_ref[...] = acc_ref[...] * alpha + trans_dot(w.astype(jnp.bfloat16), keys[:lat])
            return carry

        lax.fori_loop(0, counts[r], step, 0)
        out_ref[r] = (acc_ref[...] / l_ref[:, :1]).astype(out_ref.dtype)


def decode_pallas(info, query, fresh, spans, cache, lat, heads, width, blk=512, depth=4):
    owned, rows, kv = query.shape
    return pl.pallas_call(
        functools.partial(
            decode_kernel,
            lat=lat,
            heads=heads,
            blk=blk,
            depth=depth,
            scale=math.log2(math.e) / math.sqrt(width),
        ),
        out_shape=jax.ShapeDtypeStruct((owned, rows, lat), jnp.bfloat16),
        in_specs=[
            pl.BlockSpec(memory_space=pltpu.SMEM),
            pl.BlockSpec(memory_space=pltpu.VMEM),
            pl.BlockSpec(memory_space=pltpu.VMEM),
            pl.BlockSpec(memory_space=pl.ANY),
            pl.BlockSpec(memory_space=pl.ANY),
        ],
        out_specs=pl.BlockSpec(memory_space=pltpu.VMEM),
        scratch_shapes=[
            pltpu.VMEM((owned, depth, kv, blk), jnp.bfloat16),
            pltpu.SemaphoreType.DMA((owned, depth)),
            pltpu.VMEM((rows, 128), jnp.float32),
            pltpu.VMEM((rows, 128), jnp.float32),
            pltpu.VMEM((rows, lat), jnp.float32),
        ],
        compiler_params=pltpu.CompilerParams(vmem_limit_bytes=40 << 20),
        cost_estimate=pl.CostEstimate(
            flops=5 * 10**9, bytes_accessed=10 << 20, transcendentals=2 << 20
        ),
    )(info, query, fresh, spans, cache)


def absorb_into(dq_ref, kw_ref, out_ref, flat, wide, heads, lat, step):
    rows = dq_ref.shape[0]
    flat[...] = dq_ref[:, :128].astype(jnp.float32)
    count = rows // heads
    for h in range(heads):
        mine = flat[pl.ds(h, count, stride=heads), :].astype(jnp.bfloat16)
        res = trans_dot(mine, kw_ref[:, h * 128 : (h + 1) * 128])
        for c in range(lat // 128):
            wide[c, pl.ds(h, count, stride=heads), :] = res[:, c * 128 : (c + 1) * 128]
    for c in range(lat // 128):
        out_ref[:, c * 128 : (c + 1) * 128] = wide[c].astype(jnp.bfloat16)
    out_ref[:, lat:] = dq_ref[:, 128:]


def absorb_kernel(dq_ref, kw_ref, out_ref, flat, wide, *, heads, lat):
    absorb_into(dq_ref, kw_ref, out_ref, flat, wide, heads, lat, 1)


def absorb_pallas(flat_queries, key_weight, heads):
    rows, width = flat_queries.shape
    lat = key_weight.shape[0]
    vm = pl.BlockSpec(memory_space=pltpu.VMEM)
    return pl.pallas_call(
        functools.partial(absorb_kernel, heads=heads, lat=lat),
        out_shape=jax.ShapeDtypeStruct((rows, lat + width - 128), jnp.bfloat16),
        in_specs=[vm, vm],
        out_specs=vm,
        scratch_shapes=[
            pltpu.VMEM((rows, 128), jnp.float32),
            pltpu.VMEM((lat // 128, rows, 128), jnp.float32),
        ],
        compiler_params=pltpu.CompilerParams(vmem_limit_bytes=24 << 20),
    )(flat_queries, key_weight)


def project_into(x_ref, vw_ref, out_ref, wide, heads, lat):
    rows = x_ref.shape[0]
    count = rows // heads
    for c in range(lat // 128):
        wide[c] = x_ref[:, c * 128 : (c + 1) * 128].astype(jnp.float32)
    for h in range(heads):
        mine = jnp.concatenate(
            [wide[c, pl.ds(h, count, stride=heads), :] for c in range(lat // 128)], axis=1
        ).astype(jnp.bfloat16)
        out_ref[:, h * 128 : (h + 1) * 128] = jnp.dot(
            mine, vw_ref[:, h * 128 : (h + 1) * 128], preferred_element_type=jnp.float32
        ).astype(jnp.bfloat16)


def project_kernel(x_ref, vw_ref, out_ref, wide, *, heads, lat):
    project_into(x_ref, vw_ref, out_ref, wide, heads, lat)


def project_pallas(flat_latent, value_weight, heads):
    rows, lat = flat_latent.shape
    vm = pl.BlockSpec(memory_space=pltpu.VMEM)
    return pl.pallas_call(
        functools.partial(project_kernel, heads=heads, lat=lat),
        out_shape=jax.ShapeDtypeStruct((rows // heads, heads * 128), jnp.bfloat16),
        in_specs=[vm, vm],
        out_specs=vm,
        scratch_shapes=[pltpu.VMEM((lat // 128, rows, 128), jnp.float32)],
        compiler_params=pltpu.CompilerParams(vmem_limit_bytes=24 << 20),
    )(flat_latent, value_weight)


def on_device(
    latent_rows,
    pre_queries,
    pre_lengths,
    owner_map,
    context_cache,
    context_lengths,
    new_latent,
    dec_queries,
    key_weight,
    value_weight,
):
    steps, rows_local, heads, width = dec_queries.shape
    if heads % 16 or latent_rows.shape[0] % 128:
        return plain_on_device(
            latent_rows,
            pre_queries,
            pre_lengths,
            owner_map,
            context_cache,
            context_lengths,
            new_latent,
            dec_queries,
            key_weight,
            value_weight,
        )
    head_rank = lax.axis_index("head")
    batch_rank = lax.axis_index("batch")
    ranks = lax.axis_size("head")
    span_len = pre_queries.shape[0]
    kv = latent_rows.shape[1]
    lat = key_weight.shape[0]
    owned = context_cache.shape[0]
    span_lengths = lax.dynamic_index_in_dim(pre_lengths, batch_rank, 0, keepdims=False)
    flat_owner, flat_start, flat_length = request_table(pre_lengths, owner_map, span_len)
    row_ids = batch_rank * rows_local + head_rank * owned + jnp.arange(owned, dtype=jnp.int32)
    matches = (flat_owner[None, :] == row_ids[:, None]).astype(jnp.int32)
    is_target = jnp.sum(matches, axis=1)
    first_row = jnp.sum(matches * flat_start[None, :], axis=1)
    prompt_len = jnp.sum(matches * flat_length[None, :], axis=1)
    first_row = lax.rem(first_row + batch_rank * span_len, 2 * span_len) * is_target
    effective = jnp.where(is_target > 0, prompt_len, context_lengths)
    info = jnp.stack([is_target, first_row, effective])
    fresh = jnp.pad(
        jnp.transpose(new_latent, (1, 0, 2)), ((0, 0), (0, 128 - steps), (0, 0))
    )
    absorbed = absorb_pallas(dec_queries.reshape(-1, width), key_weight, heads)
    query_all = absorbed.reshape(steps, rows_local, heads, kv)
    turned = jnp.transpose(latent_rows)
    half = kv // 2
    upper = lax.all_gather(turned[:half], "head", axis=0)
    turned, upper = lax.optimization_barrier((turned, upper))
    lower = lax.all_gather(turned[half:], "head", axis=0)
    own_span = jnp.concatenate([upper, lower], axis=1)
    other_span = from_partner(own_span, "batch", 0)
    all_spans = jnp.concatenate([own_span, other_span], axis=0)
    got = lax.all_to_all(query_all, "head", split_axis=1, concat_axis=2, tiled=True)
    query = jnp.transpose(got, (1, 0, 2, 3)).reshape(owned, steps * ranks * heads, kv)
    latent_out = decode_pallas(
        info, query, fresh, all_spans, jnp.transpose(context_cache, (0, 2, 1)), lat, ranks * heads, width
    )
    back = jnp.transpose(latent_out.reshape(owned, steps, ranks * heads, lat), (1, 0, 2, 3))
    returned = lax.all_to_all(back, "head", split_axis=2, concat_axis=1, tiled=True)
    prefill_out = prefill_pallas(own_span, pre_queries, span_lengths, key_weight, value_weight)
    decode_out = project_pallas(returned.reshape(-1, lat), value_weight, heads)
    return (prefill_out, decode_out.reshape(steps, rows_local, heads * 128))


def solution(mesh):
    placed = (
        P(("groups", "batch", "head"), None),
        P(("groups", "batch"), "head", None),
        P("groups", None),
        P("groups", None),
        P(("groups", "batch", "head"), None, None),
        P(("groups", "batch", "head")),
        P("groups", ("batch", "head"), None),
        P("groups", "batch", "head", None),
        P(None, "head"),
        P(None, "head"),
    )
    return jax.shard_map(
        on_device,
        mesh=mesh,
        in_specs=placed,
        out_specs=(P(("groups", "batch"), "head"), P("groups", "batch", "head")),
        check_vma=False,
    )
```
